32 devices in a mesh: role: 4 (over y, x), ep: 4 (over z), dp: 2 (over core).
Axes of the slice: x: 2, y: 2, z: 4, core: 2. Of those that a mesh axis runs over, the one named last changes fastest.
Arguments:
- latents: bfloat16 [16, 256, 1536], P(('role', 'dp'), 'ep'), may hold values from -6 to 6
- noise: bfloat16 [1, 16, 256, 1536], P(None, ('role', 'dp'), 'ep'), may hold values from -6 to 6
- expert_ids: int32 [1, 16, 256, 6], P(None, ('role', 'dp'), 'ep'), may hold values from 0 to 63, all different within a row; in each aligned block of 64 rows (0 to 63, 64 to 127, ..., all dimensions but the last counted through in order) at most 7 rows name the same one
- gate_values: float32 [1, 16, 256, 6], P(None, ('role', 'dp'), 'ep'), may hold values from 0.1 to 1
- advantages: float32 [16], P(('role', 'dp')), may hold values from -4 to 4
- expert_pair: bfloat16 [64, 2, 768, 1536], P('ep', None, ('role', 'dp')), may hold values from -6 to 6
Outputs:
- final_latents: bfloat16 [16, 256, 1536], P(('role', 'dp'), 'ep')
- new_down: bfloat16 [64, 768, 1536], P('ep')
The draws below stay inside these ranges and needn't reach their ends.
Inputs may be any that keep to these rules, and one draw needn't show every extreme that they name: `expert_ids`: each row names 6 different experts. In every aligned block of 64 rows (steps, images and tokens taken together in order; one index of ep holds one block of an image at a step) no expert is named more than 7 times, a bound that some block reaches.
All inputs are finite; a program needn't handle non-finite values.
Results may differ from the reference program's by a relative error of at most 0.008.
Values may be sent and summed in bfloat16 or wider, within the bound.
No kernel may reach another device: no remote copies, remote signals or barrier semaphores. Data moves between devices by JAX's collectives and lax.ppermute only.
A program may use at most 256 MiB of HBM per device.

```python
import math
import jax
import jax.numpy as jnp
import numpy as np
from jax import lax

D = 1536
HID = 768
EXPERTS = 64
TOP = 6
STEPS = 1
TOK_DEV = 64
IMG_DEV = 2
CAP = 7
IMG_TOK = 256
IMAGES = 16
N_EP = 4


def levels(key, shape, pieces, low, largest):
    def one(dim, parts):
        heights = jax.random.uniform(jax.random.fold_in(jax.random.fold_in(key, 6), dim), (parts,), jnp.float32, low / len(pieces), largest / len(pieces))
        return jnp.repeat(jnp.exp(heights), shape[dim] // parts).reshape((-1,) + (1,) * (len(shape) - dim - 1))

    gain = one(*pieces[0])
    for cut in pieces[1:]:
        gain = gain * one(*cut)
    return gain


def shared_out(key, own, number, rows, number_of, top, bound, lean):
    ranking = jax.random.permutation(key, number_of)
    heavy_load, common = shares(number_of, rows * top, bound, lean, True), shares(number_of, rows * top, bound, lean, False)
    places = jnp.arange(number_of)

    def named(lengths, offset_by):
        used = int((lengths > 0).sum())
        fixed = max(1, used // 4)
        passed = fixed + (places - fixed + offset_by * (used - fixed)) % max(1, number_of - fixed)
        return jnp.zeros((number_of,), jnp.int32).at[ranking[jnp.where(places < fixed, places, passed)]].set(jnp.asarray(lengths, jnp.int32))

    lengths = jnp.where(number % 4 == 0, named(heavy_load, number // 4), named(common, number - number // 4 - 1))
    mixed = jax.random.permutation(jax.random.fold_in(own, 3), number_of)
    source_of, sink = mixed[0:number_of // 2 * 2:2], mixed[1:number_of // 2 * 2:2]
    room = jnp.minimum(lengths[source_of] - 1, bound - lengths[sink]) // 2
    room = jnp.where((source_of == ranking[0]) | (sink == ranking[0]) | (lengths[sink] == 0), 0, jnp.maximum(room, 0))
    passed = jax.random.randint(jax.random.fold_in(own, 4), (number_of // 2,), 0, 1 << 20) % (room + 1)
    lengths = lengths.at[source_of].add(-passed).at[sink].add(passed)
    members = jnp.searchsorted(jnp.cumsum(lengths), jnp.arange(rows * top), side="right").astype(jnp.int32)
    grid = members.reshape(top, rows).T
    grid = grid[jax.random.permutation(jax.random.fold_in(own, 1), rows)]
    offset_by = jax.random.randint(jax.random.fold_in(own, 2), (rows, 1), 0, top)
    return jnp.take_along_axis(grid, (jnp.arange(top)[None, :] + offset_by) % top, axis=1)


def shares(count, total, limit, slope, full):
    weights = [(1 << 20) // math.isqrt(rank ** slope) + 1 for rank in range(1, count + 1)]
    largest = limit if full else min(limit, max(-(-total // count), total * weights[0] // sum(weights)))
    least = 1 if total - largest >= count - 1 else 0
    holding, rest = [largest] + [least] * (count - 1), total - largest - least * (count - 1)
    while rest > 0:
        movable = [i for i in range(1, count) if holding[i] < largest] or [i for i in range(1, count) if holding[i] < limit]
        whole, budget = sum([weights[i] for i in movable]), rest
        for i in movable:
            addition = min(limit - holding[i], max(1, budget * weights[i] // whole), rest)
            holding[i] = holding[i] + addition
            rest = rest - addition
    return np.array(holding)


def gaussian(stream_key, extent, deviation, bound, pieces=(), kind=jnp.bfloat16):
    values = deviation * jax.random.normal(stream_key, extent, jnp.float32)
    if pieces:
        values = values * levels(stream_key, extent, pieces, -0.22, 0.18)
    return jnp.clip(values, -bound, bound).astype(kind)


def setup_inputs(seed: int = 0) -> dict:
    keys = jax.random.split(jax.random.key(seed), 7)
    latents = gaussian(keys[0], (IMAGES, IMG_TOK, D), 1.0, 6.0, ((0, 8), (1, 4)))
    noise = gaussian(keys[1], (STEPS, IMAGES, IMG_TOK, D), 1.0, 6.0, ((1, 8), (2, 4)))
    expert_ids_keys = jax.random.split(jax.random.fold_in(keys[2], 1), STEPS * IMAGES * IMG_TOK // TOK_DEV)
    expert_ids_turns = jax.random.permutation(jax.random.fold_in(keys[2], 3), STEPS * IMAGES * IMG_TOK // TOK_DEV)
    expert_ids = jax.vmap(lambda own, number: shared_out(jax.random.fold_in(keys[2], 2), own, number, TOK_DEV, EXPERTS, TOP, CAP, 2))(expert_ids_keys, expert_ids_turns).reshape((STEPS, IMAGES, IMG_TOK, TOP))
    gate_values = jnp.clip(jnp.exp(math.log(1.0) - 2.3025851 * jax.random.uniform(keys[3], (STEPS, IMAGES, IMG_TOK, TOP), jnp.float32) ** levels(keys[3], (STEPS, IMAGES, IMG_TOK, TOP), ((1, 8), (2, 4)), -0.2, 0.2)), 0.1, 1.0)
    advantages = gaussian(keys[4], (IMAGES,), 1.0, 4.0, ((0, 8),), jnp.float32)
    expert_pair = gaussian(keys[5], (EXPERTS, 2, HID, D), 1.0, 6.0, ((0, 4), (2, 8)))
    return dict(latents=latents, noise=noise, expert_ids=expert_ids, gate_values=gate_values, advantages=advantages, expert_pair=expert_pair)


def coefficients(section):
    moment = 0.95 - 0.4 * section
    noise_level = 0.3 * math.sqrt(moment / (1.0 - moment))
    factor = noise_level * noise_level / (2.0 * moment)
    keep_gain = 1.0 - 0.4 * factor
    drift_gain = -0.4 * (1.0 + factor * (1.0 - moment))
    noise_gain = noise_level * math.sqrt(0.4)
    return (keep_gain, drift_gain, noise_gain)

def slot_tables(picked, weights):
    images = picked.shape[0]
    blocks = picked.reshape(images, N_EP, TOK_DEV * TOP).astype(jnp.int32)
    onehot = (blocks[..., None] == jnp.arange(EXPERTS, dtype=jnp.int32)).astype(jnp.int32)
    ranks = jnp.cumsum(onehot, axis=2).astype(jnp.int32) - 1
    placed = lax.optimization_barrier(jnp.sum(ranks * onehot, axis=3)).astype(jnp.int32)
    source = jnp.arange(N_EP, dtype=jnp.int32)[None, :, None]
    column = jnp.broadcast_to(source * CAP + placed, blocks.shape).astype(jnp.int32)
    token_pos = (jnp.arange(TOK_DEV * TOP, dtype=jnp.int32) // TOP)[None, None, :]
    token_ids = jnp.broadcast_to(source * TOK_DEV + token_pos, blocks.shape).astype(jnp.int32)
    image_ids = jnp.broadcast_to(jnp.arange(images, dtype=jnp.int32)[:, None, None], blocks.shape)
    table_token = jnp.full((images, EXPERTS, N_EP * CAP), IMG_TOK, jnp.int32)
    table_token = table_token.at[image_ids, blocks, column].set(token_ids)
    table_gate = jnp.zeros((images, EXPERTS, N_EP * CAP), jnp.float32)
    table_gate = table_gate.at[image_ids, blocks, column].set(weights.reshape(blocks.shape))
    return (jnp.transpose(table_token, (1, 0, 2)), jnp.transpose(table_gate, (1, 0, 2)))

def expert_hidden(slot_rows, w_up):
    pre_act = jnp.einsum('imd,hd->imh', slot_rows.astype(jnp.float32), w_up.astype(jnp.float32)) * (1.0 / math.sqrt(D))
    return jax.nn.gelu(pre_act, approximate=True).astype(jnp.bfloat16)

def with_sentinel(values):
    images = values.shape[0]
    return jnp.concatenate([values, jnp.zeros((images, 1, values.shape[2]), values.dtype)], axis=1)

def advance(latent, noise_now, table_token, table_gate, up_all, down_all, section):
    images = latent.shape[0]
    padded = with_sentinel(latent)
    image_index = jnp.arange(images, dtype=jnp.int32)[:, None]

    def one_expert(total, inputs):
        w_up, w_down, token_table, gate_table = inputs
        slot_rows = padded[image_index, token_table]
        hidden = expert_hidden(slot_rows, w_up)
        output = jnp.einsum('imh,hd->imd', hidden.astype(jnp.float32), w_down.astype(jnp.float32)) * (1.0 / math.sqrt(HID))
        output = output.astype(jnp.bfloat16)
        total = total.at[image_index, token_table].add(gate_table[..., None] * output.astype(jnp.float32))
        return (total, None)
    start = jnp.zeros((images, IMG_TOK + 1, D), jnp.float32)
    velocity, unused = lax.scan(one_expert, start, (up_all, down_all, table_token, table_gate))
    keep_gain, drift_gain, noise_gain = coefficients(section)
    moved = keep_gain * latent.astype(jnp.float32) + drift_gain * velocity[:, :IMG_TOK] + noise_gain * noise_now.astype(jnp.float32)
    return moved.astype(jnp.bfloat16)

def reference(latents, noise, expert_ids, gate_values, advantages, expert_pair):
    up_all = expert_pair[:, 0]
    down_all = expert_pair[:, 1]
    tables = [slot_tables(expert_ids[section], gate_values[section]) for section in range(STEPS)]
    history = [latents]
    current = latents
    for section in range(STEPS):
        current = advance(current, noise[section], tables[section][0], tables[section][1], up_all, down_all, section)
        history.append(current)
    images = latents.shape[0]
    image_index = jnp.arange(images, dtype=jnp.int32)[:, None]
    padded_latent = [with_sentinel(history[section]) for section in range(STEPS)]
    padded_noise = [with_sentinel(noise[section]) for section in range(STEPS)]
    scales = []
    for section in range(STEPS):
        keep_gain, drift_gain, noise_gain = coefficients(section)
        scales.append(advantages * (drift_gain / noise_gain))
    token_tables = jnp.stack([tables[section][0] for section in range(STEPS)], axis=1)
    gate_tables = jnp.stack([tables[section][1] for section in range(STEPS)], axis=1)
    rate = 10.0 / math.sqrt(IMG_TOK * TOP * images / EXPERTS)

    def one_expert(carry, inputs):
        w_up, w_down, token_table, gate_table = inputs
        partial_value = jnp.zeros((images, HID, D), jnp.float32)
        for section in range(STEPS):
            slot_rows = padded_latent[section][image_index, token_table[section]]
            hidden = expert_hidden(slot_rows, w_up)
            slot_scale = gate_table[section] * scales[section][:, None]
            slot_noise = padded_noise[section][image_index, token_table[section]]
            cotangent = (slot_scale[..., None] * slot_noise.astype(jnp.float32)).astype(jnp.bfloat16)
            partial_value = partial_value + jnp.einsum('imh,imd->ihd', hidden.astype(jnp.float32), cotangent.astype(jnp.float32))
        grouped = lax.optimization_barrier(jnp.sum(partial_value.reshape(images // IMG_DEV, IMG_DEV, HID, D), axis=1))
        grouped = grouped * (1.0 / math.sqrt(HID))
        rounded = lax.optimization_barrier(grouped.astype(jnp.bfloat16)).astype(jnp.float32)
        updated = (w_down.astype(jnp.float32) + rate * lax.optimization_barrier(jnp.sum(rounded, axis=0))).astype(jnp.bfloat16)
        return (carry, updated)
    unused, new_down = lax.scan(one_expert, jnp.zeros((), jnp.float32), (up_all, down_all, token_tables, gate_tables))
    return (current, new_down)
```

```python
import math

import jax
import jax.numpy as jnp
from jax import lax
from jax.experimental import pallas as pl
from jax.experimental.pallas import tpu as pltpu
from jax.sharding import PartitionSpec as P

CAP = 7


def coefficients(section):
    moment = 0.95 - 0.4 * section
    noise_level = 0.3 * math.sqrt(moment / (1.0 - moment))
    factor = noise_level * noise_level / (2.0 * moment)
    keep_gain = 1.0 - 0.4 * factor
    drift_gain = -0.4 * (1.0 + factor * (1.0 - moment))
    noise_gain = noise_level * math.sqrt(0.4)
    return (keep_gain, drift_gain, noise_gain)


def slot_matrices(picked, weights, experts, capacity):
    image_count, tokens, chosen_count = picked.shape
    flat_ids = picked.reshape(image_count, tokens * chosen_count)
    onehot = (flat_ids[..., None] == jnp.arange(experts, dtype=jnp.int32)).astype(jnp.int32)
    ranks = jnp.cumsum(onehot, axis=1) - 1
    placed = jnp.sum(ranks * onehot, axis=2)
    image_column = jnp.arange(image_count, dtype=jnp.int32)[:, None]
    slot_ids = (flat_ids * image_count + image_column) * capacity + placed
    slot_ids = slot_ids.reshape(image_count * tokens, chosen_count)
    total_slots = experts * image_count * capacity
    marked = (slot_ids[..., None] == jnp.arange(total_slots, dtype=jnp.int32)).astype(jnp.float32)
    selected = jnp.sum(marked, axis=1)
    flat_weights = weights.reshape(image_count * tokens, chosen_count)
    slot_gate = jnp.sum(jnp.sum(marked * flat_weights[..., None], axis=1), axis=0)
    return (slot_ids, selected, slot_gate, flat_weights)


def expert_pass(inputs, w_up, w_down):
    width = inputs.shape[-1]
    hidden_units = w_up.shape[1]
    pre_act = jnp.einsum("jlcd,lhd->jlch", inputs, w_up, preferred_element_type=jnp.float32) * (
        1.0 / math.sqrt(width)
    )
    hidden = jax.nn.gelu(pre_act, approximate=True).astype(jnp.bfloat16)
    output = jnp.einsum("jlch,lhd->jlcd", hidden, w_down, preferred_element_type=jnp.float32) * (
        1.0 / math.sqrt(hidden_units)
    )
    returned = lax.all_to_all(
        output.astype(jnp.bfloat16), "ep", split_axis=0, concat_axis=0, tiled=True
    )
    return (returned, hidden)


def slot_plan(latents, noise, expert_ids, gate_values, advantages, expert_pair):
    ep_size = lax.axis_size("ep")
    group_size = lax.axis_size("role") * lax.axis_size("dp")
    local_experts = expert_pair.shape[0]
    experts = local_experts * ep_size
    capacity = CAP
    image_count = latents.shape[0]
    tok_count = latents.shape[1]
    width = latents.shape[2]
    top_count = expert_ids.shape[3]
    total_slots = experts * image_count * capacity
    full_pair = lax.all_gather(expert_pair, ("role", "dp"), axis=2, tiled=True)
    w_up = full_pair[:, 0]
    w_down = full_pair[:, 1]
    hidden_units = full_pair.shape[2]
    current = latents.reshape(image_count * tok_count, width)
    image_of_slot = jnp.arange(total_slots, dtype=jnp.int32) // capacity % image_count
    keep_gain, drift_gain, noise_gain = coefficients(0)
    slot_ids, selected, slot_gate, flat_weights = slot_matrices(
        expert_ids[0], gate_values[0], experts, capacity
    )
    selected_half = selected.astype(jnp.bfloat16)
    noise_now = noise[0].reshape(image_count * tok_count, width)
    slot_latent = jnp.einsum(
        "ts,td->sd", selected_half, current, preferred_element_type=jnp.float32
    )
    slot_latent = slot_latent.astype(jnp.bfloat16).reshape(
        ep_size, local_experts, image_count * capacity, width
    )
    slot_noise = jnp.einsum(
        "ts,td->sd", selected_half, noise_now, preferred_element_type=jnp.float32
    )
    image_factor = advantages * (drift_gain / noise_gain)
    slot_scale = slot_gate * image_factor[image_of_slot]
    home_cot = (
        (slot_scale[:, None] * slot_noise)
        .astype(jnp.bfloat16)
        .reshape(ep_size, local_experts, image_count * capacity, width)
    )
    returned, hidden = expert_pass(
        lax.all_to_all(slot_latent, "ep", split_axis=0, concat_axis=0, tiled=True), w_up, w_down
    )
    returned, hidden, cotangent = (
        returned,
        hidden,
        lax.all_to_all(home_cot, "ep", split_axis=0, concat_axis=0, tiled=True),
    )
    back_rows = returned.reshape(total_slots, width)
    taken = jnp.take(back_rows, slot_ids, axis=0)
    velocity = jnp.sum(flat_weights[..., None] * taken.astype(jnp.float32), axis=1)
    moved = (
        keep_gain * current.astype(jnp.float32)
        + drift_gain * velocity
        + noise_gain * noise_now.astype(jnp.float32)
    )
    current = moved.astype(jnp.bfloat16)
    kept_hidden = [hidden]
    kept_cot = [cotangent]
    rate = 10.0 / math.sqrt(tok_count * ep_size * top_count * image_count * group_size / experts)
    share_rows = expert_pair.shape[2]
    total = jnp.zeros(
        (lax.axis_size(("role", "dp")) * share_rows, local_experts, width), jnp.float32
    )
    for hidden, cotangent in zip(kept_hidden, kept_cot):
        total = jnp.einsum("jlch,jlcd->hld", hidden, cotangent, preferred_element_type=jnp.float32)
    share = lax.psum_scatter(
        (total * (1.0 / math.sqrt(hidden_units)))
        .reshape(lax.axis_size(("role", "dp")) * share_rows, local_experts * width)
        .astype(jnp.bfloat16),
        ("role", "dp"),
        scatter_dimension=0,
        tiled=True,
    ).astype(jnp.float32)
    share = jnp.transpose(share.reshape(share_rows, local_experts, width), (1, 0, 2))
    own_down = expert_pair[:, 1].astype(jnp.float32)
    new_part = (own_down + rate * share).astype(jnp.bfloat16)
    new_down = lax.all_gather(new_part, ("role", "dp"), axis=1, tiled=True)
    return (current.reshape(image_count, tok_count, width), new_down)


def hidden_kernel(x_ref, gate_ref, up_ref, down_ref, act_ref, vel_ref, *, units, in_scale, out_scale, chunk):
    rows = x_ref.shape[0]
    columns = chunk * units
    total = up_ref.shape[0]
    x = x_ref[...]
    lane = lax.broadcasted_iota(jnp.int32, (rows, columns), 1)
    for start in range(0, total, columns):
        pre = lax.dot_general(
            x, up_ref[start : start + columns], (((1,), (1,)), ((), ())),
            preferred_element_type=jnp.float32,
        ) * in_scale
        hidden = jax.nn.gelu(pre, approximate=True).astype(jnp.bfloat16).astype(jnp.float32)
        first = start // units
        gate = jnp.broadcast_to(gate_ref[:, first : first + 1], (rows, columns))
        for k in range(1, chunk):
            gate = jnp.where(lane >= k * units, gate_ref[:, first + k : first + k + 1], gate)
        act_ref[:, start : start + columns] = (hidden * gate).astype(jnp.bfloat16)
    part = jnp.dot(act_ref[...], down_ref[...], preferred_element_type=jnp.float32) * out_scale
    part = part.astype(jnp.bfloat16)
    _, inner, _, tokens, _ = vel_ref.shape
    cores = vel_ref.shape[0]
    for j in range(inner):
        for c in range(cores):
            base = (j * cores + c) * tokens
            vel_ref[c, j, 0] = part[base : base + tokens]


def expert_chunk(experts, units):
    chunk = 1
    while chunk < experts and (chunk * units) % 128:
        chunk *= 2
    return chunk


def token_plan(latents, noise, expert_ids, gate_values, advantages, expert_pair):
    every = ("role", "ep", "dp")
    roles = lax.axis_size("role")
    eps = lax.axis_size("ep")
    cores = lax.axis_size("dp")
    devices = roles * eps * cores
    local_experts, _, units, width = expert_pair.shape
    image_count, tok_count, _ = latents.shape
    tokens = image_count * tok_count
    top_count = expert_ids.shape[3]
    hidden_units = units * roles * cores
    rows_all = tokens * devices
    keep_gain, drift_gain, noise_gain = coefficients(0)
    current = latents.reshape(tokens, width)
    noise_now = noise[0].reshape(tokens, width)
    factor = jnp.repeat(advantages * (drift_gain / noise_gain), tok_count)
    scaled_noise = (factor[:, None] * noise_now.astype(jnp.float32)).astype(jnp.bfloat16)

    picks = jnp.concatenate(
        [
            expert_ids[0].reshape(tokens, top_count).astype(jnp.float32).T,
            gate_values[0].reshape(tokens, top_count).T,
        ],
        axis=0,
    )
    x_all = lax.all_gather(current, every, axis=0, tiled=True)
    picks_all = lax.all_gather(picks, every, axis=0)
    noise_all = lax.all_gather(scaled_noise, every, axis=0, tiled=True)
    ids_all = picks_all[:, :top_count].astype(jnp.int32)
    own = lax.axis_index("ep") * local_experts + jnp.arange(local_experts, dtype=jnp.int32)
    match = ids_all[..., None] == own
    gates = jnp.sum(jnp.where(match, picks_all[:, top_count:][..., None], 0.0), axis=1)
    gates = gates.reshape(rows_all, local_experts)

    w_up = expert_pair[:, 0].reshape(local_experts * units, width)
    w_down = expert_pair[:, 1].reshape(local_experts * units, width)
    inner = 2 if eps % 2 == 0 else 1
    tile = inner * cores * tokens
    steps_ep = eps // inner
    chunk = expert_chunk(local_experts, units)
    act, part = pl.pallas_call(
        lambda *refs: hidden_kernel(
            *refs, units=units, in_scale=1.0 / math.sqrt(width),
            out_scale=1.0 / math.sqrt(hidden_units), chunk=chunk,
        ),
        grid=(rows_all // tile,),
        in_specs=[
            pl.BlockSpec((tile, width), lambda i: (i, 0)),
            pl.BlockSpec((tile, local_experts), lambda i: (i, 0)),
            pl.BlockSpec((local_experts * units, width), lambda i: (0, 0)),
            pl.BlockSpec((local_experts * units, width), lambda i: (0, 0)),
        ],
        out_specs=[
            pl.BlockSpec((tile, local_experts * units), lambda i: (i, 0)),
            pl.BlockSpec(
                (cores, inner, 1, tokens, width), lambda i: (0, i % steps_ep, i // steps_ep, 0, 0)
            ),
        ],
        out_shape=[
            jax.ShapeDtypeStruct((rows_all, local_experts * units), jnp.bfloat16),
            jax.ShapeDtypeStruct((cores, eps, roles, tokens, width), jnp.bfloat16),
        ],
        compiler_params=pltpu.CompilerParams(
            dimension_semantics=("arbitrary",), vmem_limit_bytes=56 * 1024 * 1024
        ),
        cost_estimate=pl.CostEstimate(
            flops=4 * rows_all * width * local_experts * units,
            bytes_accessed=6 * rows_all * width,
            transcendentals=rows_all * local_experts * units,
        ),
        name="hidden_and_part",
    )(x_all, gates, w_up, w_down)

    rate = 10.0 / math.sqrt(tok_count * eps * top_count * image_count * roles * cores / (local_experts * eps))
    total = lax.dot_general(act, noise_all, (((0,), (0,)), ((), ())), preferred_element_type=jnp.float32)
    new_part = w_down.astype(jnp.float32) + (rate / math.sqrt(hidden_units)) * total
    new_part = new_part.astype(jnp.bfloat16).reshape(local_experts, units, width)
    new_down = lax.all_gather(new_part, ("role", "dp"), axis=1, tiled=True)

    for name in ("dp", "ep", "role"):
        swapped = lax.all_to_all(part, name, split_axis=0, concat_axis=0, tiled=True)
        velocity = jnp.sum(swapped.astype(jnp.float32), axis=0)
        part = velocity.astype(jnp.bfloat16)
    moved = (
        keep_gain * current.astype(jnp.float32)
        + drift_gain * velocity
        + noise_gain * noise_now.astype(jnp.float32)
    )
    return (moved.astype(jnp.bfloat16).reshape(latents.shape), new_down)


def per_device(latents, noise, expert_ids, gate_values, advantages, expert_pair):
    devices = lax.axis_size(("role", "ep", "dp"))
    groups = lax.axis_size(("role", "dp"))
    images = latents.shape[0] * groups
    all_tokens = latents.shape[0] * latents.shape[1] * devices
    slots = expert_pair.shape[0] * images * lax.axis_size("ep") * CAP
    plan = token_plan if all_tokens <= slots else slot_plan
    return plan(latents, noise, expert_ids, gate_values, advantages, expert_pair)


def solution(mesh):
    in_specs = (
        P(("role", "dp"), "ep", None),
        P(None, ("role", "dp"), "ep", None),
        P(None, ("role", "dp"), "ep", None),
        P(None, ("role", "dp"), "ep", None),
        P(("role", "dp")),
        P("ep", None, ("role", "dp"), None),
    )
    out_specs = (P(("role", "dp"), "ep", None), P("ep", None, None))
    return jax.shard_map(
        per_device, mesh=mesh, in_specs=in_specs, out_specs=out_specs, check_vma=False
    )
```

```python
import math

import jax
import jax.numpy as jnp
from jax import lax
from jax.experimental import pallas as pl
from jax.experimental.pallas import tpu as pltpu
from jax.sharding import PartitionSpec as P


CAP = 7
VMEM_BYTES = 56 * 1024 * 1024


def coefficients(section):
    moment = 0.95 - 0.4 * section
    noise_level = 0.3 * math.sqrt(moment / (1.0 - moment))
    factor = noise_level * noise_level / (2.0 * moment)
    keep_gain = 1.0 - 0.4 * factor
    drift_gain = -0.4 * (1.0 + factor * (1.0 - moment))
    noise_gain = noise_level * math.sqrt(0.4)
    return (keep_gain, drift_gain, noise_gain)


def slot_matrices(picked, weights, experts, capacity):
    image_count, tokens, chosen_count = picked.shape
    flat_ids = picked.reshape(image_count, tokens * chosen_count)
    onehot = (flat_ids[..., None] == jnp.arange(experts, dtype=jnp.int32)).astype(jnp.int32)
    ranks = jnp.cumsum(onehot, axis=1) - 1
    placed = jnp.sum(ranks * onehot, axis=2)
    image_column = jnp.arange(image_count, dtype=jnp.int32)[:, None]
    slot_ids = (flat_ids * image_count + image_column) * capacity + placed
    slot_ids = slot_ids.reshape(image_count * tokens, chosen_count)
    total_slots = experts * image_count * capacity
    marked = (slot_ids[..., None] == jnp.arange(total_slots, dtype=jnp.int32)).astype(jnp.float32)
    selected = jnp.sum(marked, axis=1)
    flat_weights = weights.reshape(image_count * tokens, chosen_count)
    slot_gate = jnp.sum(jnp.sum(marked * flat_weights[..., None], axis=1), axis=0)
    return (slot_ids, selected, slot_gate, flat_weights)


def expert_pass(inputs, w_up, w_down):
    width = inputs.shape[-1]
    hidden_units = w_up.shape[1]
    pre_act = jnp.einsum("jlcd,lhd->jlch", inputs, w_up, preferred_element_type=jnp.float32) * (
        1.0 / math.sqrt(width)
    )
    hidden = jax.nn.gelu(pre_act, approximate=True).astype(jnp.bfloat16)
    output = jnp.einsum("jlch,lhd->jlcd", hidden, w_down, preferred_element_type=jnp.float32) * (
        1.0 / math.sqrt(hidden_units)
    )
    returned = lax.all_to_all(
        output.astype(jnp.bfloat16), "ep", split_axis=0, concat_axis=0, tiled=True
    )
    return (returned, hidden)


def slot_plan(latents, noise, expert_ids, gate_values, advantages, expert_pair):
    ep_size = lax.axis_size("ep")
    group_size = lax.axis_size("role") * lax.axis_size("dp")
    local_experts = expert_pair.shape[0]
    experts = local_experts * ep_size
    capacity = CAP
    image_count = latents.shape[0]
    tok_count = latents.shape[1]
    width = latents.shape[2]
    top_count = expert_ids.shape[3]
    total_slots = experts * image_count * capacity
    full_pair = lax.all_gather(expert_pair, ("role", "dp"), axis=2, tiled=True)
    w_up = full_pair[:, 0]
    w_down = full_pair[:, 1]
    hidden_units = full_pair.shape[2]
    current = latents.reshape(image_count * tok_count, width)
    image_of_slot = jnp.arange(total_slots, dtype=jnp.int32) // capacity % image_count
    keep_gain, drift_gain, noise_gain = coefficients(0)
    slot_ids, selected, slot_gate, flat_weights = slot_matrices(
        expert_ids[0], gate_values[0], experts, capacity
    )
    selected_half = selected.astype(jnp.bfloat16)
    noise_now = noise[0].reshape(image_count * tok_count, width)
    slot_latent = jnp.einsum(
        "ts,td->sd", selected_half, current, preferred_element_type=jnp.float32
    )
    slot_latent = slot_latent.astype(jnp.bfloat16).reshape(
        ep_size, local_experts, image_count * capacity, width
    )
    slot_noise = jnp.einsum(
        "ts,td->sd", selected_half, noise_now, preferred_element_type=jnp.float32
    )
    image_factor = advantages * (drift_gain / noise_gain)
    slot_scale = slot_gate * image_factor[image_of_slot]
    home_cot = (
        (slot_scale[:, None] * slot_noise)
        .astype(jnp.bfloat16)
        .reshape(ep_size, local_experts, image_count * capacity, width)
    )
    returned, hidden = expert_pass(
        lax.all_to_all(slot_latent, "ep", split_axis=0, concat_axis=0, tiled=True), w_up, w_down
    )
    returned, hidden, cotangent = (
        returned,
        hidden,
        lax.all_to_all(home_cot, "ep", split_axis=0, concat_axis=0, tiled=True),
    )
    back_rows = returned.reshape(total_slots, width)
    taken = jnp.take(back_rows, slot_ids, axis=0)
    velocity = jnp.sum(flat_weights[..., None] * taken.astype(jnp.float32), axis=1)
    moved = (
        keep_gain * current.astype(jnp.float32)
        + drift_gain * velocity
        + noise_gain * noise_now.astype(jnp.float32)
    )
    current = moved.astype(jnp.bfloat16)
    kept_hidden = [hidden]
    kept_cot = [cotangent]
    rate = 10.0 / math.sqrt(tok_count * ep_size * top_count * image_count * group_size / experts)
    share_rows = expert_pair.shape[2]
    total = jnp.zeros(
        (lax.axis_size(("role", "dp")) * share_rows, local_experts, width), jnp.float32
    )
    for hidden, cotangent in zip(kept_hidden, kept_cot):
        total = jnp.einsum("jlch,jlcd->hld", hidden, cotangent, preferred_element_type=jnp.float32)
    share = lax.psum_scatter(
        (total * (1.0 / math.sqrt(hidden_units)))
        .reshape(lax.axis_size(("role", "dp")) * share_rows, local_experts * width)
        .astype(jnp.bfloat16),
        ("role", "dp"),
        scatter_dimension=0,
        tiled=True,
    ).astype(jnp.float32)
    share = jnp.transpose(share.reshape(share_rows, local_experts, width), (1, 0, 2))
    own_down = expert_pair[:, 1].astype(jnp.float32)
    new_part = (own_down + rate * share).astype(jnp.bfloat16)
    new_down = lax.all_gather(new_part, ("role", "dp"), axis=1, tiled=True)
    return (current.reshape(image_count, tok_count, width), new_down)


def swap(x, axis, bit):
    return lax.ppermute(x, axis, [(i, i ^ bit) for i in range(lax.axis_size(axis))])


def from_ahead(x, step):
    size = lax.axis_size("ep")
    return lax.ppermute(x, "ep", [((i + step) % size, i) for i in range(size)])


def to_ahead(x, step):
    size = lax.axis_size("ep")
    return lax.ppermute(x, "ep", [(i, (i + step) % size) for i in range(size)])


def plane_neighbours(block):
    return swap(block, "role", 1), swap(block, "role", 2)


def plane_diagonal(first, second):
    half = first.shape[0] // 2
    return swap(first[:half], "role", 2), swap(second[half:], "role", 1)


def spread_along(rows):
    return [from_ahead(rows, step) for step in range(1, lax.axis_size("ep"))]


def near_layout(count):
    half = count // 2
    copies = [(n, 0, count, n * count) for n in range(3)]
    return copies + [(3, 0, half, 3 * count), (4, 0, half, 3 * count + half)]


def far_layout(count, steps):
    copies = []
    half = steps * count // 2
    for s in range(steps):
        low, high = s * count, (s + 1) * count
        base = 4 * low
        copies += [(n, low, count, base + n * count) for n in range(3)]
        if low < half:
            copies.append((3, low, min(high, half) - low, base + 3 * count))
        if high > half:
            start = max(low, half)
            copies.append((4, start - half, high - start, base + 3 * count + start - low))
    return copies


def piece_copies(pieces, target, sems, layout, offset=0):
    return [
        pltpu.make_async_copy(
            pieces[n].at[pl.ds(first, size)], target.at[pl.ds(offset + start, size)], sems.at[k]
        )
        for k, (n, first, size, start) in enumerate(layout)
    ]


def hidden_kernel(*refs, layout, width, columns, in_scale, out_scale):
    pieces = refs[:-7]
    up_ref, down_ref, pick_ref, act_ref, part_ref, x_ref, sems = refs[-7:]
    tile = act_ref.shape[0]
    step = pl.program_id(0)
    copies = piece_copies(pieces, x_ref, sems, layout)

    @pl.when(step == 0)
    def _():
        for copy in copies:
            copy.start()

    for k in range(x_ref.shape[0] // tile):

        @pl.when(step == k)
        def _(k=k):
            for copy, entry in zip(copies, layout):
                if entry[3] // tile == k:
                    copy.wait()

    rows = pl.ds(pl.multiple_of(step * tile, tile), tile)
    x = x_ref[rows, :width]
    gates = x_ref[rows, width:]
    for start in range(0, up_ref.shape[0], columns):
        pre = lax.dot_general(
            x, up_ref[start : start + columns], (((1,), (1,)), ((), ())),
            preferred_element_type=jnp.float32,
        ) * in_scale
        hidden = jax.nn.gelu(pre, approximate=True).astype(jnp.bfloat16).astype(jnp.float32)
        gate = jnp.dot(gates, pick_ref[:, start : start + columns], preferred_element_type=jnp.float32)
        act_ref[:, start : start + columns] = (hidden * gate).astype(jnp.bfloat16)
    part = jnp.dot(act_ref[...], down_ref[...], preferred_element_type=jnp.float32) * out_scale
    part_ref[...] = part.astype(jnp.bfloat16)


def column_span(total):
    for parts in (4, 3, 2):
        if total % (parts * 128) == 0:
            return total // parts
    return total


def hidden_and_part(pieces, layout, gate_width, w_up, w_down, pick, hidden_units, tile):
    total, width = w_up.shape
    count = sum(entry[2] for entry in layout)
    return pl.pallas_call(
        lambda *refs: hidden_kernel(
            *refs, layout=layout, width=width, columns=column_span(total),
            in_scale=1.0 / math.sqrt(width), out_scale=1.0 / math.sqrt(hidden_units),
        ),
        grid=(count // tile,),
        in_specs=[pl.BlockSpec(memory_space=pl.ANY)] * len(pieces)
        + [
            pl.BlockSpec((total, width), lambda i: (0, 0)),
            pl.BlockSpec((total, width), lambda i: (0, 0)),
            pl.BlockSpec((gate_width, total), lambda i: (0, 0)),
        ],
        out_specs=[
            pl.BlockSpec((tile, total), lambda i: (i, 0)),
            pl.BlockSpec((tile, width), lambda i: (i, 0)),
        ],
        out_shape=[
            jax.ShapeDtypeStruct((count, total), jnp.bfloat16),
            jax.ShapeDtypeStruct((count, width), jnp.bfloat16),
        ],
        scratch_shapes=[
            pltpu.VMEM((count, width + gate_width), jnp.bfloat16),
            pltpu.SemaphoreType.DMA((len(layout),)),
        ],
        compiler_params=pltpu.CompilerParams(
            dimension_semantics=("arbitrary",), vmem_limit_bytes=VMEM_BYTES
        ),
        cost_estimate=pl.CostEstimate(
            flops=4 * count * width * total,
            bytes_accessed=6 * count * width + 4 * total * width,
            transcendentals=count * total,
        ),
        name="hidden_and_part",
    )(*pieces, w_up, w_down, pick)


def update_kernel(*refs, layouts, scale):
    groups = len(layouts)
    pieces = refs[: 5 * groups]
    acts = refs[5 * groups : 6 * groups]
    down_ref, out_ref, noise_ref, sems = refs[6 * groups :]
    counts = [sum(entry[2] for entry in layout) for layout in layouts]
    offsets = [sum(counts[:g]) for g in range(groups)]

    @pl.when(pl.program_id(0) == 0)
    def _():
        copies = []
        for g in range(groups):
            copies += piece_copies(
                pieces[5 * g : 5 * g + 5], noise_ref, sems.at[g], layouts[g], offsets[g]
            )
        for copy in copies:
            copy.start()
        for copy in copies:
            copy.wait()

    total = jnp.zeros(out_ref.shape, jnp.float32)
    for g in range(groups):
        total = total + lax.dot_general(
            acts[g][...], noise_ref[offsets[g] : offsets[g] + counts[g]], (((0,), (0,)), ((), ())),
            preferred_element_type=jnp.float32,
        )
    out_ref[...] = (down_ref[...].astype(jnp.float32) + scale * total).astype(jnp.bfloat16)


def updated_rows(pieces, layouts, acts, w_down, scale, columns, first, steps):
    counts = [sum(entry[2] for entry in layout) for layout in layouts]
    rows = sum(counts)
    width = w_down.shape[1]
    flat = [piece for group in pieces for piece in group]
    return pl.pallas_call(
        lambda *refs: update_kernel(*refs, layouts=layouts, scale=scale),
        grid=(steps,),
        in_specs=[pl.BlockSpec(memory_space=pl.ANY)] * len(flat)
        + [
            pl.BlockSpec((count, columns), lambda i, block=block: (block, first + i))
            for count, (_, block) in zip(counts, acts)
        ]
        + [pl.BlockSpec((columns, width), lambda i: (first + i, 0))],
        out_specs=pl.BlockSpec((columns, width), lambda i: (i, 0)),
        out_shape=jax.ShapeDtypeStruct((steps * columns, width), jnp.bfloat16),
        scratch_shapes=[
            pltpu.VMEM((rows, width), jnp.bfloat16),
            pltpu.SemaphoreType.DMA((len(layouts), max(len(layout) for layout in layouts))),
        ],
        compiler_params=pltpu.CompilerParams(
            dimension_semantics=("arbitrary",), vmem_limit_bytes=VMEM_BYTES
        ),
        cost_estimate=pl.CostEstimate(
            flops=2 * rows * width * columns * steps,
            bytes_accessed=2 * rows * width + 8 * columns * steps * width,
            transcendentals=0,
        ),
        name="updated_rows",
    )(*flat, *[act for act, _ in acts], w_down)


def place_kernel(*refs, first, starts, cores):
    pieces = refs[: len(starts)]
    out, held, in_sems, out_sems = refs[-4:]
    role = lax.axis_index("role")
    core = lax.axis_index("dp")
    loads, stores = [], []
    row = 0
    for n, (offset, role_bit, core_bit) in enumerate(starts):
        slot = (role ^ role_bit) * cores + (core ^ core_bit)
        size = pieces[n].shape[0]
        room = held.at[pl.ds(row, size)]
        loads.append(pltpu.make_async_copy(pieces[n], room, in_sems.at[n]))
        stores.append(
            pltpu.make_async_copy(room, out.at[pl.ds(first + offset, size), slot], out_sems.at[n])
        )
        row += size
    for load in loads:
        load.start()
    for load, store in zip(loads, stores):
        load.wait()
        store.start()
    for store in stores:
        store.wait()


def place(out, pieces, first, starts, shape, cores):
    operands = list(pieces) + ([] if out is None else [out])
    rows = sum(piece.shape[0] for piece in pieces)
    return pl.pallas_call(
        lambda *refs: place_kernel(*refs, first=first, starts=starts, cores=cores),
        in_specs=[pl.BlockSpec(memory_space=pl.ANY)] * len(operands),
        out_specs=pl.BlockSpec(memory_space=pl.ANY),
        out_shape=jax.ShapeDtypeStruct(shape, jnp.bfloat16),
        scratch_shapes=[
            pltpu.VMEM((rows,) + shape[2:], jnp.bfloat16),
            pltpu.SemaphoreType.DMA((len(pieces),)),
            pltpu.SemaphoreType.DMA((len(pieces),)),
        ],
        input_output_aliases={} if out is None else {len(pieces): 0},
        compiler_params=pltpu.CompilerParams(vmem_limit_bytes=VMEM_BYTES),
        name="place",
    )(*operands)


def other_core(pieces):
    return [swap(piece, "dp", 1) for piece in pieces]


def token_plan(latents, noise, expert_ids, gate_values, advantages, expert_pair):
    roles = lax.axis_size("role")
    eps = lax.axis_size("ep")
    cores = lax.axis_size("dp")
    local_experts, _, units, width = expert_pair.shape
    experts = local_experts * eps
    image_count, tok_count, _ = latents.shape
    tokens = image_count * tok_count
    top_count = expert_ids.shape[3]
    hidden_units = units * roles * cores
    gate_width = 2 * experts
    keep_gain, drift_gain, noise_gain = coefficients(0)
    current = latents.reshape(tokens, width)
    noise_now = noise[0].reshape(tokens, width)
    factor = jnp.repeat(advantages * (drift_gain / noise_gain), tok_count)
    scaled_noise = (factor[:, None] * noise_now.astype(jnp.float32)).astype(jnp.bfloat16)

    ids = expert_ids[0].reshape(tokens, top_count)
    values = gate_values[0].reshape(tokens, top_count)
    match = ids[..., None] == jnp.arange(experts, dtype=jnp.int32)
    table = jnp.sum(jnp.where(match, values[..., None], 0.0), axis=1)
    table_high = lax.reduce_precision(table, 8, 7)
    table_low = table - table_high
    rows = jnp.concatenate(
        [current, table_high.astype(jnp.bfloat16), table_low.astype(jnp.bfloat16)], axis=1
    )
    own = lax.axis_index("ep") * local_experts + jnp.arange(local_experts * units, dtype=jnp.int32) // units
    source = jnp.arange(gate_width, dtype=jnp.int32) % experts
    pick = (source[:, None] == own[None, :]).astype(jnp.bfloat16)
    w_up = expert_pair[:, 0].reshape(local_experts * units, width)
    w_down = expert_pair[:, 1].reshape(local_experts * units, width)
    tile = roles * tokens
    close = near_layout(tokens)
    distant = far_layout(tokens, eps - 1)

    def hidden(pieces, layout):
        return hidden_and_part(pieces, layout, gate_width, w_up, w_down, pick, hidden_units, tile)

    row_along = spread_along(rows)
    row_near = [rows, *plane_neighbours(rows)]
    row_near += plane_diagonal(*row_near[1:])
    row_near_there = other_core(row_near)
    scaled_noise, row_along = lax.optimization_barrier((scaled_noise, row_along))
    noise_along = spread_along(scaled_noise)
    row_stack = jnp.concatenate(row_along, axis=0)
    row_far = [row_stack, *plane_neighbours(row_stack)]
    row_far += plane_diagonal(*row_far[1:])
    row_far_there = other_core(row_far)
    both = close + [(5 + n, first, size, tile + start) for n, first, size, start in close]
    act_near, part_near = hidden(row_near + row_near_there, both)

    noise_stack = jnp.concatenate(noise_along, axis=0)
    held = lax.optimization_barrier((scaled_noise, noise_stack, row_far[1], row_far[2]))
    noise_far = [held[1], *plane_neighbours(held[1])]
    noise_near = [held[0], *plane_neighbours(held[0])]
    act_far_here, part_far_here = hidden(row_far, distant)
    noise_far += plane_diagonal(*noise_far[1:])
    noise_near += plane_diagonal(*noise_near[1:])
    near_early = other_core(noise_near[:3])
    far_early = other_core(noise_far[:3])
    act_far_there, part_far_there = hidden(row_far_there, distant)
    noise_near_there = near_early + other_core(noise_near[3:])
    noise_far_there = far_early + other_core(noise_far[3:])

    line = part_near[:tile].astype(jnp.float32)
    line = line + swap(part_near[tile:], "dp", 1).astype(jnp.float32)
    pair = part_far_here.astype(jnp.float32) + swap(part_far_there, "dp", 1).astype(jnp.float32)
    pair = pair.astype(jnp.bfloat16).reshape(eps - 1, roles * tokens, width)
    back = [to_ahead(pair[step - 1], step) for step in range(1, eps)]
    for piece in back:
        line = line + piece.astype(jnp.float32)
    line = line.reshape(roles, tokens, width)
    velocity = line[0]
    for bit in range(1, roles):
        velocity = velocity + swap(line[bit].astype(jnp.bfloat16), "role", bit).astype(jnp.float32)
    moved = (
        keep_gain * current.astype(jnp.float32)
        + drift_gain * velocity
        + noise_gain * noise_now.astype(jnp.float32)
    )

    rate = 10.0 / math.sqrt(tok_count * eps * top_count * image_count * roles * cores / experts)
    step_scale = rate / math.sqrt(hidden_units)
    shape = (local_experts, roles * cores, units, width)
    chunks = 4
    chunk = local_experts // chunks
    columns = chunk * units
    acts = ((act_near, 0), (act_far_here, 0), (act_near, 1), (act_far_there, 0))
    noises = (noise_near, noise_far, noise_near_there, noise_far_there)
    layouts = (close, distant, close, distant)
    head = updated_rows(noises, layouts, acts, w_down, step_scale, columns, 0, 1)
    rest = updated_rows(noises, layouts, acts, w_down, step_scale, columns, 1, chunks - 1)
    new_down = None
    waiting = []
    sent = []
    starts = [(0, 0, 0), (0, 1, 0), (0, 2, 0), (0, 3, 0), (chunk // 2, 3, 0)]
    starts += [(offset, bit, 1) for offset, bit, _ in starts]
    for c in range(chunks):
        last = c == chunks - 1
        mine = head if c == 0 else rest[(c - 1) * columns : c * columns]
        mine = mine.reshape(chunk, units, width)

        def place_next(value):
            nonlocal new_down
            n, pieces = waiting.pop(0)
            new_down = place(new_down, pieces, n * chunk, starts, shape, cores)
            value, new_down = lax.optimization_barrier((value, new_down))
            return value

        if len(sent) >= 2:
            mine, _ = lax.optimization_barrier((mine, sent[-2]))
        near = plane_neighbours(mine)
        sent.append(near)
        early = other_core([mine, *near])
        if last:
            near = place_next(near)
        diagonal = plane_diagonal(*near)
        if last:
            diagonal = place_next(diagonal)
        late = other_core(diagonal)
        if last:
            late = place_next(late)
        waiting.append((c, [mine, *near, *diagonal, *early, *late]))
    n, pieces = waiting.pop(0)
    new_down = place(new_down, pieces, n * chunk, starts, shape, cores)
    new_down = new_down.reshape(local_experts, hidden_units, width)
    return (moved.astype(jnp.bfloat16).reshape(latents.shape), new_down)


def per_device(latents, noise, expert_ids, gate_values, advantages, expert_pair):
    devices = lax.axis_size(("role", "ep", "dp"))
    groups = lax.axis_size(("role", "dp"))
    local_experts, _, units, width = expert_pair.shape
    experts = local_experts * lax.axis_size("ep")
    images = latents.shape[0] * groups
    all_tokens = latents.shape[0] * latents.shape[1] * devices
    slots = experts * images * CAP
    fits = (
        all_tokens <= slots
        and lax.axis_size("role") == 4
        and lax.axis_size("dp") == 2
        and local_experts % 8 == 0
        and (local_experts // 4 * units) % 128 == 0
        and (latents.shape[0] * latents.shape[1]) % 32 == 0
        and (2 * experts) % 128 == 0
        and width % (2 * experts) == 0
        and (local_experts * units) % 128 == 0
    )
    if not fits:
        return slot_plan(latents, noise, expert_ids, gate_values, advantages, expert_pair)
    return token_plan(latents, noise, expert_ids, gate_values, advantages, expert_pair)


def solution(mesh):
    in_specs = (
        P(("role", "dp"), "ep", None),
        P(None, ("role", "dp"), "ep", None),
        P(None, ("role", "dp"), "ep", None),
        P(None, ("role", "dp"), "ep", None),
        P(("role", "dp")),
        P("ep", None, ("role", "dp"), None),
    )
    out_specs = (P(("role", "dp"), "ep", None), P("ep", None, None))
    return jax.shard_map(
        per_device, mesh=mesh, in_specs=in_specs, out_specs=out_specs, check_vma=False
    )
```

```python
import math

import jax
import jax.numpy as jnp
from jax import lax
from jax.experimental import pallas as pl
from jax.experimental.pallas import tpu as pltpu
from jax.sharding import PartitionSpec as P


CAP = 7
VMEM_BYTES = 56 * 1024 * 1024


def coefficients(section):
    moment = 0.95 - 0.4 * section
    noise_level = 0.3 * math.sqrt(moment / (1.0 - moment))
    factor = noise_level * noise_level / (2.0 * moment)
    keep_gain = 1.0 - 0.4 * factor
    drift_gain = -0.4 * (1.0 + factor * (1.0 - moment))
    noise_gain = noise_level * math.sqrt(0.4)
    return (keep_gain, drift_gain, noise_gain)


def slot_matrices(picked, weights, experts, capacity):
    image_count, tokens, chosen_count = picked.shape
    flat_ids = picked.reshape(image_count, tokens * chosen_count)
    onehot = (flat_ids[..., None] == jnp.arange(experts, dtype=jnp.int32)).astype(jnp.int32)
    ranks = jnp.cumsum(onehot, axis=1) - 1
    placed = jnp.sum(ranks * onehot, axis=2)
    image_column = jnp.arange(image_count, dtype=jnp.int32)[:, None]
    slot_ids = (flat_ids * image_count + image_column) * capacity + placed
    slot_ids = slot_ids.reshape(image_count * tokens, chosen_count)
    total_slots = experts * image_count * capacity
    marked = (slot_ids[..., None] == jnp.arange(total_slots, dtype=jnp.int32)).astype(jnp.float32)
    selected = jnp.sum(marked, axis=1)
    flat_weights = weights.reshape(image_count * tokens, chosen_count)
    slot_gate = jnp.sum(jnp.sum(marked * flat_weights[..., None], axis=1), axis=0)
    return (slot_ids, selected, slot_gate, flat_weights)


def expert_pass(inputs, w_up, w_down):
    width = inputs.shape[-1]
    hidden_units = w_up.shape[1]
    pre_act = jnp.einsum("jlcd,lhd->jlch", inputs, w_up, preferred_element_type=jnp.float32) * (
        1.0 / math.sqrt(width)
    )
    hidden = jax.nn.gelu(pre_act, approximate=True).astype(jnp.bfloat16)
    output = jnp.einsum("jlch,lhd->jlcd", hidden, w_down, preferred_element_type=jnp.float32) * (
        1.0 / math.sqrt(hidden_units)
    )
    returned = lax.all_to_all(
        output.astype(jnp.bfloat16), "ep", split_axis=0, concat_axis=0, tiled=True
    )
    return (returned, hidden)


def slot_plan(latents, noise, expert_ids, gate_values, advantages, expert_pair):
    ep_size = lax.axis_size("ep")
    group_size = lax.axis_size("role") * lax.axis_size("dp")
    local_experts = expert_pair.shape[0]
    experts = local_experts * ep_size
    capacity = CAP
    image_count = latents.shape[0]
    tok_count = latents.shape[1]
    width = latents.shape[2]
    top_count = expert_ids.shape[3]
    total_slots = experts * image_count * capacity
    full_pair = lax.all_gather(expert_pair, ("role", "dp"), axis=2, tiled=True)
    w_up = full_pair[:, 0]
    w_down = full_pair[:, 1]
    hidden_units = full_pair.shape[2]
    current = latents.reshape(image_count * tok_count, width)
    image_of_slot = jnp.arange(total_slots, dtype=jnp.int32) // capacity % image_count
    keep_gain, drift_gain, noise_gain = coefficients(0)
    slot_ids, selected, slot_gate, flat_weights = slot_matrices(
        expert_ids[0], gate_values[0], experts, capacity
    )
    selected_half = selected.astype(jnp.bfloat16)
    noise_now = noise[0].reshape(image_count * tok_count, width)
    slot_latent = jnp.einsum(
        "ts,td->sd", selected_half, current, preferred_element_type=jnp.float32
    )
    slot_latent = slot_latent.astype(jnp.bfloat16).reshape(
        ep_size, local_experts, image_count * capacity, width
    )
    slot_noise = jnp.einsum(
        "ts,td->sd", selected_half, noise_now, preferred_element_type=jnp.float32
    )
    image_factor = advantages * (drift_gain / noise_gain)
    slot_scale = slot_gate * image_factor[image_of_slot]
    home_cot = (
        (slot_scale[:, None] * slot_noise)
        .astype(jnp.bfloat16)
        .reshape(ep_size, local_experts, image_count * capacity, width)
    )
    returned, hidden = expert_pass(
        lax.all_to_all(slot_latent, "ep", split_axis=0, concat_axis=0, tiled=True), w_up, w_down
    )
    returned, hidden, cotangent = (
        returned,
        hidden,
        lax.all_to_all(home_cot, "ep", split_axis=0, concat_axis=0, tiled=True),
    )
    back_rows = returned.reshape(total_slots, width)
    taken = jnp.take(back_rows, slot_ids, axis=0)
    velocity = jnp.sum(flat_weights[..., None] * taken.astype(jnp.float32), axis=1)
    moved = (
        keep_gain * current.astype(jnp.float32)
        + drift_gain * velocity
        + noise_gain * noise_now.astype(jnp.float32)
    )
    current = moved.astype(jnp.bfloat16)
    kept_hidden = [hidden]
    kept_cot = [cotangent]
    rate = 10.0 / math.sqrt(tok_count * ep_size * top_count * image_count * group_size / experts)
    share_rows = expert_pair.shape[2]
    total = jnp.zeros(
        (lax.axis_size(("role", "dp")) * share_rows, local_experts, width), jnp.float32
    )
    for hidden, cotangent in zip(kept_hidden, kept_cot):
        total = jnp.einsum("jlch,jlcd->hld", hidden, cotangent, preferred_element_type=jnp.float32)
    share = lax.psum_scatter(
        (total * (1.0 / math.sqrt(hidden_units)))
        .reshape(lax.axis_size(("role", "dp")) * share_rows, local_experts * width)
        .astype(jnp.bfloat16),
        ("role", "dp"),
        scatter_dimension=0,
        tiled=True,
    ).astype(jnp.float32)
    share = jnp.transpose(share.reshape(share_rows, local_experts, width), (1, 0, 2))
    own_down = expert_pair[:, 1].astype(jnp.float32)
    new_part = (own_down + rate * share).astype(jnp.bfloat16)
    new_down = lax.all_gather(new_part, ("role", "dp"), axis=1, tiled=True)
    return (current.reshape(image_count, tok_count, width), new_down)


def swap(x, axis, bit):
    return lax.ppermute(x, axis, [(i, i ^ bit) for i in range(lax.axis_size(axis))])


def from_ahead(x, step):
    size = lax.axis_size("ep")
    return lax.ppermute(x, "ep", [((i + step) % size, i) for i in range(size)])


def to_ahead(x, step):
    size = lax.axis_size("ep")
    return lax.ppermute(x, "ep", [(i, (i + step) % size) for i in range(size)])


def plane_neighbours(block):
    return swap(block, "role", 1), swap(block, "role", 2)


def plane_diagonal(first, second):
    half = first.shape[0] // 2
    return swap(first[:half], "role", 2), swap(second[half:], "role", 1)


def spread_along(rows):
    return [from_ahead(rows, step) for step in range(1, lax.axis_size("ep"))]


def near_layout(count):
    half = count // 2
    copies = [(n, 0, count, n * count) for n in range(3)]
    return copies + [(3, 0, half, 3 * count), (4, 0, half, 3 * count + half)]


def far_layout(count, steps):
    copies = []
    half = steps * count // 2
    for s in range(steps):
        low, high = s * count, (s + 1) * count
        base = 4 * low
        copies += [(n, low, count, base + n * count) for n in range(3)]
        if low < half:
            copies.append((3, low, min(high, half) - low, base + 3 * count))
        if high > half:
            start = max(low, half)
            copies.append((4, start - half, high - start, base + 3 * count + start - low))
    return copies


def piece_copies(pieces, target, sems, layout, offset=0):
    return [
        pltpu.make_async_copy(
            pieces[n].at[pl.ds(first, size)], target.at[pl.ds(offset + start, size)], sems.at[k]
        )
        for k, (n, first, size, start) in enumerate(layout)
    ]


def hidden_kernel(*refs, layout, width, columns, in_scale, out_scale):
    pieces = refs[:-7]
    up_ref, down_ref, pick_ref, act_ref, part_ref, x_ref, sems = refs[-7:]
    tile = act_ref.shape[0]
    step = pl.program_id(0)
    copies = piece_copies(pieces, x_ref, sems, layout)

    @pl.when(step == 0)
    def _():
        for copy in copies:
            copy.start()

    for k in range(x_ref.shape[0] // tile):

        @pl.when(step == k)
        def _(k=k):
            for copy, entry in zip(copies, layout):
                if entry[3] // tile == k:
                    copy.wait()

    rows = pl.ds(pl.multiple_of(step * tile, tile), tile)
    x = x_ref[rows, :width]
    gates = x_ref[rows, width:]
    for start in range(0, up_ref.shape[0], columns):
        pre = lax.dot_general(
            x, up_ref[start : start + columns], (((1,), (1,)), ((), ())),
            preferred_element_type=jnp.float32,
        ) * in_scale
        hidden = jax.nn.gelu(pre, approximate=True).astype(jnp.bfloat16).astype(jnp.float32)
        gate = jnp.dot(gates, pick_ref[:, start : start + columns], preferred_element_type=jnp.float32)
        act_ref[:, start : start + columns] = (hidden * gate).astype(jnp.bfloat16)
    part = jnp.dot(act_ref[...], down_ref[...], preferred_element_type=jnp.float32) * out_scale
    part_ref[...] = part.astype(jnp.bfloat16)


def column_span(total):
    for parts in (4, 3, 2):
        if total % (parts * 128) == 0:
            return total // parts
    return total


def hidden_and_part(pieces, layout, gate_width, w_up, w_down, pick, hidden_units, tile):
    total, width = w_up.shape
    count = sum(entry[2] for entry in layout)
    return pl.pallas_call(
        lambda *refs: hidden_kernel(
            *refs, layout=layout, width=width, columns=column_span(total),
            in_scale=1.0 / math.sqrt(width), out_scale=1.0 / math.sqrt(hidden_units),
        ),
        grid=(count // tile,),
        in_specs=[pl.BlockSpec(memory_space=pl.ANY)] * len(pieces)
        + [
            pl.BlockSpec((total, width), lambda i: (0, 0)),
            pl.BlockSpec((total, width), lambda i: (0, 0)),
            pl.BlockSpec((gate_width, total), lambda i: (0, 0)),
        ],
        out_specs=[
            pl.BlockSpec((tile, total), lambda i: (i, 0)),
            pl.BlockSpec((tile, width), lambda i: (i, 0)),
        ],
        out_shape=[
            jax.ShapeDtypeStruct((count, total), jnp.bfloat16),
            jax.ShapeDtypeStruct((count, width), jnp.bfloat16),
        ],
        scratch_shapes=[
            pltpu.VMEM((count, width + gate_width), jnp.bfloat16),
            pltpu.SemaphoreType.DMA((len(layout),)),
        ],
        compiler_params=pltpu.CompilerParams(
            dimension_semantics=("arbitrary",), vmem_limit_bytes=VMEM_BYTES
        ),
        cost_estimate=pl.CostEstimate(
            flops=4 * count * width * total,
            bytes_accessed=6 * count * width + 4 * total * width,
            transcendentals=count * total,
        ),
        name="hidden_and_part",
    )(*pieces, w_up, w_down, pick)


def update_kernel(*refs, layouts, scale):
    groups = len(layouts)
    pieces = refs[: 5 * groups]
    acts = refs[5 * groups : 6 * groups]
    down_ref, out_ref, noise_ref, sems = refs[6 * groups :]
    counts = [sum(entry[2] for entry in layout) for layout in layouts]
    offsets = [sum(counts[:g]) for g in range(groups)]

    @pl.when(pl.program_id(0) == 0)
    def _():
        copies = []
        for g in range(groups):
            copies += piece_copies(
                pieces[5 * g : 5 * g + 5], noise_ref, sems.at[g], layouts[g], offsets[g]
            )
        for copy in copies:
            copy.start()
        for copy in copies:
            copy.wait()

    total = jnp.zeros(out_ref.shape, jnp.float32)
    for g in range(groups):
        total = total + lax.dot_general(
            acts[g][...], noise_ref[offsets[g] : offsets[g] + counts[g]], (((0,), (0,)), ((), ())),
            preferred_element_type=jnp.float32,
        )
    out_ref[...] = (down_ref[...].astype(jnp.float32) + scale * total).astype(jnp.bfloat16)


def updated_rows(pieces, layouts, acts, w_down, scale, columns, first, steps):
    counts = [sum(entry[2] for entry in layout) for layout in layouts]
    rows = sum(counts)
    width = w_down.shape[1]
    flat = [piece for group in pieces for piece in group]
    return pl.pallas_call(
        lambda *refs: update_kernel(*refs, layouts=layouts, scale=scale),
        grid=(steps,),
        in_specs=[pl.BlockSpec(memory_space=pl.ANY)] * len(flat)
        + [
            pl.BlockSpec((count, columns), lambda i, block=block: (block, first + i))
            for count, (_, block) in zip(counts, acts)
        ]
        + [pl.BlockSpec((columns, width), lambda i: (first + i, 0))],
        out_specs=pl.BlockSpec((columns, width), lambda i: (i, 0)),
        out_shape=jax.ShapeDtypeStruct((steps * columns, width), jnp.bfloat16),
        scratch_shapes=[
            pltpu.VMEM((rows, width), jnp.bfloat16),
            pltpu.SemaphoreType.DMA((len(layouts), max(len(layout) for layout in layouts))),
        ],
        compiler_params=pltpu.CompilerParams(
            dimension_semantics=("arbitrary",), vmem_limit_bytes=VMEM_BYTES
        ),
        cost_estimate=pl.CostEstimate(
            flops=2 * rows * width * columns * steps,
            bytes_accessed=2 * rows * width + 8 * columns * steps * width,
            transcendentals=0,
        ),
        name="updated_rows",
    )(*flat, *[act for act, _ in acts], w_down)


def place_kernel(*refs, first, starts, cores):
    pieces = refs[: len(starts)]
    out, held, in_sems, out_sems = refs[-4:]
    role = lax.axis_index("role")
    core = lax.axis_index("dp")
    loads, stores = [], []
    row = 0
    for n, (offset, role_bit, core_bit) in enumerate(starts):
        slot = (role ^ role_bit) * cores + (core ^ core_bit)
        size = pieces[n].shape[0]
        room = held.at[pl.ds(row, size)]
        loads.append(pltpu.make_async_copy(pieces[n], room, in_sems.at[n]))
        stores.append(
            pltpu.make_async_copy(room, out.at[pl.ds(first + offset, size), slot], out_sems.at[n])
        )
        row += size
    for load in loads:
        load.start()
    for load, store in zip(loads, stores):
        load.wait()
        store.start()
    for store in stores:
        store.wait()


def place(out, pieces, first, starts, shape, cores):
    operands = list(pieces) + ([] if out is None else [out])
    rows = sum(piece.shape[0] for piece in pieces)
    return pl.pallas_call(
        lambda *refs: place_kernel(*refs, first=first, starts=starts, cores=cores),
        in_specs=[pl.BlockSpec(memory_space=pl.ANY)] * len(operands),
        out_specs=pl.BlockSpec(memory_space=pl.ANY),
        out_shape=jax.ShapeDtypeStruct(shape, jnp.bfloat16),
        scratch_shapes=[
            pltpu.VMEM((rows,) + shape[2:], jnp.bfloat16),
            pltpu.SemaphoreType.DMA((len(pieces),)),
            pltpu.SemaphoreType.DMA((len(pieces),)),
        ],
        input_output_aliases={} if out is None else {len(pieces): 0},
        compiler_params=pltpu.CompilerParams(vmem_limit_bytes=VMEM_BYTES),
        name="place",
    )(*operands)


def other_core(pieces):
    return [swap(piece, "dp", 1) for piece in pieces]


def token_plan(latents, noise, expert_ids, gate_values, advantages, expert_pair):
    roles = lax.axis_size("role")
    eps = lax.axis_size("ep")
    cores = lax.axis_size("dp")
    local_experts, _, units, width = expert_pair.shape
    experts = local_experts * eps
    image_count, tok_count, _ = latents.shape
    tokens = image_count * tok_count
    top_count = expert_ids.shape[3]
    hidden_units = units * roles * cores
    gate_width = 2 * experts
    keep_gain, drift_gain, noise_gain = coefficients(0)
    current = latents.reshape(tokens, width)
    noise_now = noise[0].reshape(tokens, width)
    factor = jnp.repeat(advantages * (drift_gain / noise_gain), tok_count)
    scaled_noise = (factor[:, None] * noise_now.astype(jnp.float32)).astype(jnp.bfloat16)

    ids = expert_ids[0].reshape(tokens, top_count)
    values = gate_values[0].reshape(tokens, top_count)
    match = ids[..., None] == jnp.arange(experts, dtype=jnp.int32)
    table = jnp.sum(jnp.where(match, values[..., None], 0.0), axis=1)
    table_high = lax.reduce_precision(table, 8, 7)
    table_low = table - table_high
    rows = jnp.concatenate(
        [current, table_high.astype(jnp.bfloat16), table_low.astype(jnp.bfloat16)], axis=1
    )
    own = lax.axis_index("ep") * local_experts + jnp.arange(local_experts * units, dtype=jnp.int32) // units
    source = jnp.arange(gate_width, dtype=jnp.int32) % experts
    pick = (source[:, None] == own[None, :]).astype(jnp.bfloat16)
    w_up = expert_pair[:, 0].reshape(local_experts * units, width)
    w_down = expert_pair[:, 1].reshape(local_experts * units, width)
    tile = roles * tokens
    close = near_layout(tokens)
    distant = far_layout(tokens, eps - 1)

    def hidden(pieces, layout):
        return hidden_and_part(pieces, layout, gate_width, w_up, w_down, pick, hidden_units, tile)

    row_along = spread_along(rows)
    row_near = [rows, *plane_neighbours(rows)]
    row_near += plane_diagonal(*row_near[1:])
    row_near_there = other_core(row_near)
    scaled_noise, row_along = lax.optimization_barrier((scaled_noise, row_along))
    noise_along = spread_along(scaled_noise)
    row_stack = jnp.concatenate(row_along, axis=0)
    row_far = [row_stack, *plane_neighbours(row_stack)]
    row_far += plane_diagonal(*row_far[1:])
    row_far_there = other_core(row_far)
    both = close + [(5 + n, first, size, tile + start) for n, first, size, start in close]
    act_near, part_near = hidden(row_near + row_near_there, both)

    noise_stack = jnp.concatenate(noise_along, axis=0)
    held = lax.optimization_barrier((scaled_noise, noise_stack, row_far[1], row_far[2]))
    noise_far = [held[1], *plane_neighbours(held[1])]
    noise_near = [held[0], *plane_neighbours(held[0])]
    act_far_here, part_far_here = hidden(row_far, distant)
    noise_far += plane_diagonal(*noise_far[1:])
    noise_near += plane_diagonal(*noise_near[1:])
    near_early = other_core(noise_near[:3])
    far_early = other_core(noise_far[:3])
    act_far_there, part_far_there = hidden(row_far_there, distant)
    noise_near_there = near_early + other_core(noise_near[3:])
    noise_far_there = far_early + other_core(noise_far[3:])

    line = part_near[:tile].astype(jnp.float32)
    line = line + swap(part_near[tile:], "dp", 1).astype(jnp.float32)
    pair = part_far_here.astype(jnp.float32) + swap(part_far_there, "dp", 1).astype(jnp.float32)
    pair = pair.astype(jnp.bfloat16).reshape(eps - 1, roles * tokens, width)
    back = [to_ahead(pair[step - 1], step) for step in range(1, eps)]
    for piece in back:
        line = line + piece.astype(jnp.float32)
    line = line.reshape(roles, tokens, width)
    velocity = line[0]
    for bit in range(1, roles):
        velocity = velocity + swap(line[bit].astype(jnp.bfloat16), "role", bit).astype(jnp.float32)
    moved = (
        keep_gain * current.astype(jnp.float32)
        + drift_gain * velocity
        + noise_gain * noise_now.astype(jnp.float32)
    )

    rate = 10.0 / math.sqrt(tok_count * eps * top_count * image_count * roles * cores / experts)
    step_scale = rate / math.sqrt(hidden_units)
    shape = (local_experts, roles * cores, units, width)
    chunks = 4
    chunk = local_experts // chunks
    columns = chunk * units
    acts = ((act_near, 0), (act_far_here, 0), (act_near, 1), (act_far_there, 0))
    noises = (noise_near, noise_far, noise_near_there, noise_far_there)
    layouts = (close, distant, close, distant)
    head = updated_rows(noises, layouts, acts, w_down, step_scale, columns, 0, 1)
    rest = updated_rows(noises, layouts, acts, w_down, step_scale, columns, 1, chunks - 1)
    new_down = None
    sent = []
    starts = [(0, 0, 0), (0, 1, 0), (0, 2, 0), (0, 3, 0), (chunk // 2, 3, 0)]
    starts += [(offset, bit, 1) for offset, bit, _ in starts]
    for c in range(chunks):
        mine = head if c == 0 else rest[(c - 1) * columns : c * columns]
        mine = mine.reshape(chunk, units, width)
        if len(sent) >= 2:
            mine, _ = lax.optimization_barrier((mine, sent[-2]))
        near = plane_neighbours(mine)
        sent.append(near)
        diagonal = plane_diagonal(*near)
        early = other_core([mine, *near])
        late = other_core(diagonal)
        pieces = [mine, *near, *diagonal, *early, *late]
        new_down = place(new_down, pieces, c * chunk, starts, shape, cores)
    new_down = new_down.reshape(local_experts, hidden_units, width)
    return (moved.astype(jnp.bfloat16).reshape(latents.shape), new_down)


def per_device(latents, noise, expert_ids, gate_values, advantages, expert_pair):
    devices = lax.axis_size(("role", "ep", "dp"))
    groups = lax.axis_size(("role", "dp"))
    local_experts, _, units, width = expert_pair.shape
    experts = local_experts * lax.axis_size("ep")
    images = latents.shape[0] * groups
    all_tokens = latents.shape[0] * latents.shape[1] * devices
    slots = experts * images * CAP
    fits = (
        all_tokens <= slots
        and lax.axis_size("role") == 4
        and lax.axis_size("dp") == 2
        and local_experts % 8 == 0
        and (local_experts // 4 * units) % 128 == 0
        and (latents.shape[0] * latents.shape[1]) % 32 == 0
        and (2 * experts) % 128 == 0
        and width % (2 * experts) == 0
        and (local_experts * units) % 128 == 0
    )
    if not fits:
        return slot_plan(latents, noise, expert_ids, gate_values, advantages, expert_pair)
    return token_plan(latents, noise, expert_ids, gate_values, advantages, expert_pair)


def solution(mesh):
    in_specs = (
        P(("role", "dp"), "ep", None),
        P(None, ("role", "dp"), "ep", None),
        P(None, ("role", "dp"), "ep", None),
        P(None, ("role", "dp"), "ep", None),
        P(("role", "dp")),
        P("ep", None, ("role", "dp"), None),
    )
    out_specs = (P(("role", "dp"), "ep", None), P("ep", None, None))
    return jax.shard_map(
        per_device, mesh=mesh, in_specs=in_specs, out_specs=out_specs, check_vma=False
    )
```
